32 devices in a mesh: group: 2 (over x), seq: 8 (over z, y), head: 2 (over core).
Axes of the slice: x: 2, y: 2, z: 4, core: 2. Of those that a mesh axis runs over, the one named last changes fastest.
Arguments:
- queries: bfloat16 [4096, 8192], P(('group', 'seq', 'head')), parts along dimension 0, may hold values from -6 to 6
- keys: bfloat16 [4096, 1024], P(('group', 'seq', 'head')), parts along dimension 0, may hold values from -6 to 6
- values: bfloat16 [4096, 1024], P(('group', 'seq', 'head')), parts along dimension 0, may hold values from -6 to 6
- lengths: int32 [8], P('group'), parts along dimension 0, may hold values from 1 to 1024, 2048 in all
- assign: int32 [32], P('group'), parts along dimension 0, may hold values from 0 to 15, each once
Outputs:
- attended: bfloat16 [4096, 8192], P(('group', 'seq', 'head')), parts along dimension 0
The draws below stay inside these ranges and needn't reach their ends.
There are 2 independent parts, one for each index of `group`. The reference program is written for one: setup_inputs(seed, part) draws one part's arguments, and reference() takes and returns one part's arrays. A program takes and returns all parts, laid end to end along the dimension named above; each array names one. Nothing has to cross between parts.
Inputs may be any that keep to these rules, and one draw needn't show every extreme that they name: 4 positive lengths summing to 2048, the largest exactly 1024. `assign`: each span index once.
All inputs are finite; a program needn't handle non-finite values.
Results may differ from the reference program's by a relative error of at most 0.004.
Values may be sent and summed in bfloat16 or wider, within the bound.
A program may use at most 128 MiB of HBM per device.

```python
import math
import jax
import jax.numpy as jnp
import numpy as np
from jax import lax

QUERY_HEADS = 64
KEY_VALUE_HEADS = 8
HEAD_SIZE = 128
TOK_DEV = 128
DOCS = 4
SPANS = 16
PACKED_TOKENS = 2048


def draw_queries(key, part):
    base_offset = jnp.clip(jax.random.normal(jax.random.fold_in(key, 11), (PACKED_TOKENS, QUERY_HEADS * HEAD_SIZE), jnp.float32), -6.0, 6.0)
    return base_offset.astype(jnp.bfloat16)


def draw_keys(key, part):
    base_offset = jnp.clip(jax.random.normal(jax.random.fold_in(key, 12), (PACKED_TOKENS, KEY_VALUE_HEADS * HEAD_SIZE), jnp.float32), -6.0, 6.0)
    return base_offset.astype(jnp.bfloat16)


def level_of(key, shape, cuts, low, high):
    loudness, own = 1.0, jax.random.fold_in(key, 6)
    for dim, shards_of in cuts:
        draws = jnp.exp(jax.random.uniform(jax.random.fold_in(own, dim), (shards_of,), jnp.float32, low / len(cuts), high / len(cuts)))
        loudness = loudness * jnp.repeat(draws, shape[dim] // shards_of).reshape([-1 if axis == dim else 1 for axis in range(len(shape))])
    return loudness


def split_up(number_of, total, limit, slope):
    portions = [(1 << 20) // math.isqrt(rank ** slope) + 1 for rank in range(2, number_of + 1)]
    surplus, holding = total - limit - (number_of - 1), [1] * (number_of - 1)
    while surplus > 0:
        candidates = [i for i in range(number_of - 1) if holding[i] < limit]
        mass, budget = sum([portions[i] for i in candidates]), surplus
        for i in candidates:
            addition = min(limit - holding[i], max(1, budget * portions[i] // mass), surplus)
            holding[i] = holding[i] + addition
            surplus = surplus - addition
    return np.array([limit] + holding)


def ragged_sizes(own_key, number_of, total, reach, lean):
    if number_of == 2:
        one = jax.random.randint(own_key, (), max(1, total - reach), min(reach, total - 1) + 1)
        return jnp.stack([one, total - one])
    sizes = jnp.asarray(split_up(number_of, total, reach, lean), jnp.int32)
    couples = (number_of - 1) // 2
    source_of, taker = sizes[1:1 + 2 * couples:2], sizes[2:2 + 2 * couples:2]
    margin = jnp.minimum(source_of - 1, reach - taker)
    moved = jax.random.randint(jax.random.fold_in(own_key, 1), (couples,), 0, 1 << 20) % (margin + 1)
    sizes = sizes.at[1:1 + 2 * couples:2].set(source_of - moved).at[2:2 + 2 * couples:2].set(taker + moved)
    return sizes[jax.random.permutation(jax.random.fold_in(own_key, 2), number_of)]


def scatter_about(rng, shape, deviation, reach, cuts=(), kind=jnp.bfloat16):
    entries = deviation * jax.random.normal(rng, shape, jnp.float32)
    if cuts:
        entries = entries * level_of(rng, shape, cuts, -0.22, 0.18)
    return jnp.clip(entries, -reach, reach).astype(kind)


def setup_inputs(seed: int = 0, part: int = 0) -> dict:
    splits = jax.random.split(jax.random.key(seed), 6)
    own_keys = jax.random.split(jax.random.fold_in(splits[5], part), 6)
    return {
        "queries": draw_queries(jax.random.fold_in(jax.random.fold_in(splits[5], part), 71), part),
        "keys": draw_keys(jax.random.fold_in(jax.random.fold_in(splits[5], part), 71), part),
        "values": scatter_about(own_keys[2], (PACKED_TOKENS, KEY_VALUE_HEADS * HEAD_SIZE), 1.0, 6.0, ((0, 16),)),
        "lengths": ragged_sizes(own_keys[3], DOCS, PACKED_TOKENS, PACKED_TOKENS // 2, 2).astype(jnp.int32),
        "assign": jax.random.permutation(own_keys[4], SPANS).astype(jnp.int32),
    }


def reference(queries, keys, values, lengths, assign):
    rows = jnp.arange(PACKED_TOKENS, dtype=jnp.int32)
    place = assign[rows // TOK_DEV].astype(jnp.int32) * TOK_DEV + rows % TOK_DEV
    ends = jnp.cumsum(lengths).astype(jnp.int32)
    owner = jnp.sum((place[:, None] >= ends[None, :]).astype(jnp.int32), axis=1)
    visible = (owner[:, None] == owner[None, :]) & (place[None, :] <= place[:, None])
    query_group = QUERY_HEADS // KEY_VALUE_HEADS
    scale = 1.0 / (HEAD_SIZE ** 0.5)
    q_heads = queries.reshape(PACKED_TOKENS, QUERY_HEADS, HEAD_SIZE).transpose(1, 0, 2)
    key_head_rows = keys.reshape(PACKED_TOKENS, KEY_VALUE_HEADS, HEAD_SIZE).transpose(1, 0, 2)
    value_head_rows = values.reshape(PACKED_TOKENS, KEY_VALUE_HEADS, HEAD_SIZE).transpose(1, 0, 2)

    def one_head(head):
        query = q_heads[head]
        key = key_head_rows[head // query_group]
        value = value_head_rows[head // query_group]
        scores = jnp.dot(query, key.T, preferred_element_type=jnp.float32) * scale
        scores = jnp.where(visible, scores, -jnp.inf)
        top = jnp.max(scores, axis=1, keepdims=True)
        weights = jnp.exp(scores - top)
        total = jnp.sum(weights, axis=1, keepdims=True)
        return jnp.dot(weights.astype(jnp.bfloat16), value, preferred_element_type=jnp.float32) / total

    result = lax.map(one_head, jnp.arange(QUERY_HEADS, dtype=jnp.int32))
    return result.transpose(1, 0, 2).reshape(PACKED_TOKENS, QUERY_HEADS * HEAD_SIZE).astype(jnp.bfloat16)
```

```python
import functools
import math

import jax
import jax.numpy as jnp
from jax import lax
from jax.experimental import pallas as pl
from jax.experimental.pallas import tpu as pltpu
from jax.sharding import PartitionSpec as P

QUERY_HEADS = 64
KEY_VALUE_HEADS = 8
HEAD_SIZE = 128
QUERY_GROUP = QUERY_HEADS // KEY_VALUE_HEADS
MESH = pl.DeviceIdType.MESH


def ring_pos(chip, chips):
    odd = chip % 2
    return (1 - odd) * (chip // 2) + odd * ((2 * chips - 1 - chip) // 2)


def ring_chip(pos, chips):
    back = pos // (chips // 2)
    return (1 - back) * (2 * pos) + back * (2 * chips - 1 - 2 * pos)


def kernel(chips, window, docs, lengths, assign, q_hbm, k_hbm, v_hbm, out, *scratch):
    heads = KEY_VALUE_HEADS // 2
    mine = scratch[:heads]
    sib = scratch[heads : 2 * heads]
    (queries, k_win, v_win, bias, q_sem, own_sem, ring_recv, ring_send,
     sib_recv, sib_send, swap_send) = scratch[2 * heads :]
    span = queries.shape[0]
    half = chips // 2
    group = lax.axis_index("group")
    chip = lax.axis_index("seq")
    core = lax.axis_index("head")
    pos = ring_pos(chip, chips)
    other = 1 - core

    def device(p):
        return (group, ring_chip(p, chips), core)

    right = device((pos + 1) % chips)
    left = device((pos + chips - 1) % chips)
    twin = (group, chip, other)

    barrier = pltpu.get_barrier_semaphore()
    for target in (right, left, twin):
        pl.semaphore_signal(barrier, inc=1, device_id=target, device_id_type=MESH)

    def columns(index):
        return pl.ds(pl.multiple_of(index * HEAD_SIZE, HEAD_SIZE), HEAD_SIZE)

    for h in range(heads):
        for part, array in enumerate((k_hbm, v_hbm)):
            pltpu.make_async_copy(
                array.at[:, columns(core * heads + h)],
                mine[h].at[pos, part, core],
                own_sem.at[h],
            ).start()
    q_copy = pltpu.make_async_copy(q_hbm, queries, q_sem)
    pl.semaphore_wait(barrier, 3)
    for h in range(heads):
        for part, array in enumerate((k_hbm, v_hbm)):
            pltpu.make_async_remote_copy(
                array.at[:, columns(other * heads + h)],
                mine[h].at[pos, part, core],
                swap_send.at[h],
                own_sem.at[h],
                device_id=twin,
                device_id_type=MESH,
            ).start()
    q_copy.start()

    def ring_copy(h, way, step, part):
        block = (pos + chips - step + 1) % chips if way == 0 else (pos + step - 1) % chips
        return pltpu.make_async_remote_copy(
            mine[h].at[block, part],
            mine[h].at[block, part],
            ring_send.at[h],
            ring_recv.at[h, way, 2 * (step - 1) + part],
            device_id=right if way == 0 else left,
            device_id_type=MESH,
        )

    def send_own(h):
        pltpu.make_async_copy(mine[h].at[pos], mine[h].at[pos], own_sem.at[h]).wait()
        for part in range(2):
            for way in range(2):
                ring_copy(h, way, 1, part).start()

    def share(h, block, part):
        pltpu.make_async_remote_copy(
            mine[h].at[block, part],
            sib[h].at[block, part],
            sib_send.at[h],
            sib_recv.at[h],
            device_id=twin,
            device_id_type=MESH,
        ).start()

    def share_own(h):
        for part in range(2):
            share(h, pos, part)

    send_own(0)
    send_own(1)
    share_own(0)
    share_own(1)

    me = chip * 2 + core
    place = assign[me]
    slots = []
    for j in range(window):
        wanted = jnp.maximum(place - j, 0)
        found = jnp.int32(0)
        for r in range(2 * chips):
            slot = ring_pos(r // 2, chips) * 2 + r % 2
            found = found + jnp.where(assign[r] == wanted, slot, 0)
        slots.append(jnp.minimum(found, 2 * chips - 1))

    row = place * span + lax.broadcasted_iota(jnp.int32, (span, 1), 0)
    opened = jnp.zeros((span, 1), jnp.int32)
    end = jnp.int32(0)
    for d in range(docs):
        end = end + lengths[d]
        opened = jnp.where(row >= end, end, opened)
    for j in range(window):
        column = (place - j) * span + lax.broadcasted_iota(jnp.int32, (span, span), 1)
        seen = (column >= opened) & (column <= row)
        bias[:, j * span : (j + 1) * span] = jnp.where(seen, 0.0, -1e30)

    q_copy.wait()
    per = max(1, 2 * QUERY_GROUP // chips)
    chunks = QUERY_GROUP // per
    factor = math.log2(math.e) / math.sqrt(HEAD_SIZE)

    def take(buffer):
        for j in range(window):
            k_win[j * span : (j + 1) * span, :] = buffer[slots[j] // 2, 0, slots[j] % 2]
            v_win[j * span : (j + 1) * span, :] = buffer[slots[j] // 2, 1, slots[j] % 2]

    def attend(key_head, chunk):
        first = key_head * QUERY_GROUP + chunk * per
        stacked = jnp.concatenate([queries[:, columns(first + i)] for i in range(per)], axis=0)
        scores = lax.dot_general(
            stacked, k_win[...], (((1,), (1,)), ((), ())), preferred_element_type=jnp.float32
        )
        shade = bias[...]
        scores = scores * factor + jnp.concatenate([shade] * per, axis=0)
        top = jnp.max(scores, axis=1, keepdims=True)
        weights = jnp.exp2(scores - top)
        total = jnp.sum(weights, axis=1, keepdims=True)
        result = jnp.dot(
            weights.astype(jnp.bfloat16), v_win[...], preferred_element_type=jnp.float32
        )
        result = (result / total).astype(out.dtype)
        for i in range(per):
            out[:, columns(first + i)] = result[i * span : (i + 1) * span]

    def whole(buffer, sem):
        pltpu.make_async_copy(buffer, buffer, sem).wait()

    for h in range(heads + 1):
        if h < heads and h >= 1 and h + 1 < heads:
            send_own(h + 1)
            share_own(h + 1)
        if h >= 1:
            take(mine[h - 1])

        def turn(i, carry, h=h):
            if h < heads:
                step = i // 2 + 1
                part = i % 2
                for way in range(2):
                    def arrive(way=way):
                        came = (pos + chips - step) % chips if way == 0 else (pos + step) % chips
                        ring_copy(h, way, step, part).wait_recv()

                        @pl.when(i < chips - 4 + 1 if way == 0 else i < chips - 4)
                        def _():
                            ring_copy(h, way, step + 1, part).start()

                        if way == 1:
                            @pl.when(i == chips - 3)
                            def _():
                                ring_copy(h, way, step + 1, part).start()

                        share(h, came, part)

                    if way == 0:
                        pl.when(i < chips - 1)(arrive)
                    else:
                        pl.when((i < chips - 2) | (i == chips - 1))(arrive)
            if h >= 1:
                @pl.when(i == chunks)
                def _():
                    whole(sib[h - 1], sib_recv.at[h - 1])
                    take(sib[h - 1])

                twin_turn = i // chunks
                owner = (1 - twin_turn) * core + twin_turn * other
                attend(owner * heads + h - 1, i % chunks)
            return carry

        lax.fori_loop(0, chips, turn, 0)

    for h in range(heads):
        rest = mine[h].at[pl.ds(0, chips - 1)]
        pltpu.make_async_copy(rest, rest, ring_send.at[h]).wait()
        whole(mine[h], sib_send.at[h])
        swapped = mine[h].at[0, 0]
        pltpu.make_async_copy(swapped, swapped, swap_send.at[h]).wait()


def local(chips, queries, keys, values, lengths, assign):
    span = queries.shape[0]
    heads = KEY_VALUE_HEADS // 2
    window = assign.shape[0] // 2 + 1
    docs = lengths.shape[0]
    buffers = [
        pltpu.VMEM((chips, 2, 2, span, HEAD_SIZE), jnp.bfloat16) for _ in range(2 * heads)
    ]
    smem = pl.BlockSpec(memory_space=pltpu.SMEM)
    anywhere = pl.BlockSpec(memory_space=pl.ANY)
    dma = pltpu.SemaphoreType.DMA
    return pl.pallas_call(
        functools.partial(kernel, chips, window, docs),
        out_shape=jax.ShapeDtypeStruct(queries.shape, queries.dtype),
        in_specs=[smem, smem, anywhere, anywhere, anywhere],
        out_specs=pl.BlockSpec(memory_space=pltpu.VMEM),
        scratch_shapes=[
            *buffers,
            pltpu.VMEM(queries.shape, queries.dtype),
            pltpu.VMEM((window * span, HEAD_SIZE), jnp.bfloat16),
            pltpu.VMEM((window * span, HEAD_SIZE), jnp.bfloat16),
            pltpu.VMEM((span, window * span), jnp.float32),
            dma(()),
            dma((heads,)),
            dma((heads, 2, chips)),
            dma((heads,)),
            dma((heads,)),
            dma((heads,)),
            dma((heads,)),
        ],
        compiler_params=pltpu.CompilerParams(
            collective_id=0, has_side_effects=True, vmem_limit_bytes=60 * 1024 * 1024
        ),
    )(lengths, assign, queries, keys, values)


def solution(mesh):
    rows = P(("group", "seq", "head"), None)
    return jax.shard_map(
        functools.partial(local, mesh.shape["seq"]),
        mesh=mesh,
        in_specs=(rows, rows, rows, P("group"), P("group")),
        out_specs=rows,
        check_vma=False,
    )
```

```python
import functools
import math

import jax
import jax.numpy as jnp
from jax import lax
from jax.experimental import pallas as pl
from jax.experimental.pallas import tpu as pltpu
from jax.sharding import PartitionSpec as P

QUERY_HEADS = 64
KEY_VALUE_HEADS = 8
HEAD_SIZE = 128
QUERY_GROUP = QUERY_HEADS // KEY_VALUE_HEADS
MESH = pl.DeviceIdType.MESH


def ring_pos(chip, chips):
    odd = chip % 2
    return (1 - odd) * (chip // 2) + odd * ((2 * chips - 1 - chip) // 2)


def ring_chip(pos, chips):
    back = pos // (chips // 2)
    return (1 - back) * (2 * pos) + back * (2 * chips - 1 - 2 * pos)


def kernel(chips, window, docs, lengths, assign, q_hbm, k_hbm, v_hbm, out, *scratch):
    heads = KEY_VALUE_HEADS // 2
    mine = scratch[:heads]
    sib = scratch[heads : 2 * heads]
    (queries, k_win, v_win, bias, q_sem, own_sem, ring_recv, ring_send,
     sib_recv, sib_send, swap_send) = scratch[2 * heads :]
    span = queries.shape[0]
    half = chips // 2
    group = lax.axis_index("group")
    chip = lax.axis_index("seq")
    core = lax.axis_index("head")
    pos = ring_pos(chip, chips)
    other = 1 - core

    def device(p):
        return (group, ring_chip(p, chips), core)

    right = device((pos + 1) % chips)
    left = device((pos + chips - 1) % chips)
    twin = (group, chip, other)

    barrier = pltpu.get_barrier_semaphore()
    for target in (right, left, twin):
        pl.semaphore_signal(barrier, inc=1, device_id=target, device_id_type=MESH)

    def columns(index):
        return pl.ds(pl.multiple_of(index * HEAD_SIZE, HEAD_SIZE), HEAD_SIZE)

    for h in range(heads):
        for part, array in enumerate((k_hbm, v_hbm)):
            pltpu.make_async_copy(
                array.at[:, columns(core * heads + h)],
                mine[h].at[pos, part, core],
                own_sem.at[h],
            ).start()
    q_copy = pltpu.make_async_copy(q_hbm, queries, q_sem)
    pl.semaphore_wait(barrier, 3)
    for h in range(heads):
        for part, array in enumerate((k_hbm, v_hbm)):
            pltpu.make_async_remote_copy(
                array.at[:, columns(other * heads + h)],
                mine[h].at[pos, part, core],
                swap_send.at[h],
                own_sem.at[h],
                device_id=twin,
                device_id_type=MESH,
            ).start()
    q_copy.start()

    def ring_copy(h, way, step, part, piece):
        block = (pos + chips - step + 1) % chips if way == 0 else (pos + step - 1) % chips
        return pltpu.make_async_remote_copy(
            mine[h].at[block, part, piece],
            mine[h].at[block, part, piece],
            ring_send.at[h],
            ring_recv.at[h, way, 4 * (step - 1) + 2 * part + piece],
            device_id=right if way == 0 else left,
            device_id_type=MESH,
        )

    def send_own(h):
        pltpu.make_async_copy(mine[h].at[pos], mine[h].at[pos], own_sem.at[h]).wait()
        for part in range(2):
            for piece in range(2):
                for way in range(2):
                    ring_copy(h, way, 1, part, piece).start()

    def share(h, block, part, piece):
        pltpu.make_async_remote_copy(
            mine[h].at[block, part, piece],
            sib[h].at[block, part, piece],
            sib_send.at[h],
            sib_recv.at[h],
            device_id=twin,
            device_id_type=MESH,
        ).start()

    def share_own(h):
        for part in range(2):
            for piece in range(2):
                share(h, pos, part, piece)

    send_own(0)
    send_own(1)
    share_own(0)
    share_own(1)

    me = chip * 2 + core
    place = assign[me]
    slots = []
    for j in range(window):
        wanted = jnp.maximum(place - j, 0)
        found = jnp.int32(0)
        for r in range(2 * chips):
            slot = ring_pos(r // 2, chips) * 2 + r % 2
            found = found + jnp.where(assign[r] == wanted, slot, 0)
        slots.append(jnp.minimum(found, 2 * chips - 1))

    row = place * span + lax.broadcasted_iota(jnp.int32, (span, 1), 0)
    opened = jnp.zeros((span, 1), jnp.int32)
    end = jnp.int32(0)
    for d in range(docs):
        end = end + lengths[d]
        opened = jnp.where(row >= end, end, opened)
    for j in range(window):
        column = (place - j) * span + lax.broadcasted_iota(jnp.int32, (span, span), 1)
        seen = (column >= opened) & (column <= row)
        bias[:, j * span : (j + 1) * span] = jnp.where(seen, 0.0, -1e30)

    q_copy.wait()
    turns = chips // 2
    per = QUERY_GROUP // turns
    factor = math.log2(math.e) / math.sqrt(HEAD_SIZE)

    def take(buffer, place_of):
        for j in range(window):
            at = slice(j * span, (j + 1) * span)
            k_win[place_of, at, :] = buffer[slots[j] // 2, 0, slots[j] % 2]
            v_win[place_of, at, :] = buffer[slots[j] // 2, 1, slots[j] % 2]

    def attend(h, chunk):
        starts = [(owner * heads + h) * QUERY_GROUP + chunk * per for owner in (core, other)]
        shade = jnp.concatenate([bias[...]] * per, axis=0)
        results = []
        for place_of, first in enumerate(starts):
            stacked = jnp.concatenate([queries[:, columns(first + i)] for i in range(per)], axis=0)
            scores = lax.dot_general(
                stacked, k_win[place_of], (((1,), (1,)), ((), ())),
                preferred_element_type=jnp.float32,
            )
            scores = scores * factor + shade
            top = jnp.max(scores, axis=1, keepdims=True)
            weights = jnp.exp2(scores - top)
            total = jnp.sum(weights, axis=1, keepdims=True)
            result = jnp.dot(
                weights.astype(jnp.bfloat16), v_win[place_of], preferred_element_type=jnp.float32
            )
            results.append((result / total).astype(out.dtype))
        for first, result in zip(starts, results):
            for i in range(per):
                out[:, columns(first + i)] = result[i * span : (i + 1) * span]

    def whole(buffer, sem):
        pltpu.make_async_copy(buffer, buffer, sem).wait()

    def relay(h, i):
        step = i // 2 + 1
        part = i % 2

        def arrive(way, piece):
            came = (pos + chips - step) % chips if way == 0 else (pos + step) % chips
            ring_copy(h, way, step, part, piece).wait_recv()
            onward = i < chips - 3 if way == 0 else (i < chips - 4) | (i == chips - 3)

            @pl.when(onward)
            def _():
                ring_copy(h, way, step + 1, part, piece).start()

            share(h, came, part, piece)

        for piece in range(2):
            pl.when(i < chips - 1)(functools.partial(arrive, 0, piece))
            pl.when((i < chips - 2) | (i == chips - 1))(functools.partial(arrive, 1, piece))

    for phase in range(heads + 2):

        def turn(i, carry, phase=phase):
            if 1 <= phase <= heads:
                relay(phase - 1, i + turns)
            if phase < heads:
                relay(phase, i)
            if phase + 2 < heads:
                @pl.when(i == turns // 2)
                def _():
                    send_own(phase + 2)
                    share_own(phase + 2)
            if phase >= 2:
                @pl.when(i == 0)
                def _():
                    take(mine[phase - 2], 0)
                    whole(sib[phase - 2], sib_recv.at[phase - 2])
                    take(sib[phase - 2], 1)

                attend(phase - 2, i)
            return carry

        lax.fori_loop(0, turns, turn, 0)

    for h in range(heads):
        rest = mine[h].at[pl.ds(0, chips - 1)]
        pltpu.make_async_copy(rest, rest, ring_send.at[h]).wait()
        whole(mine[h], sib_send.at[h])
        swapped = mine[h].at[0, 0]
        pltpu.make_async_copy(swapped, swapped, swap_send.at[h]).wait()


def local(chips, queries, keys, values, lengths, assign):
    span = queries.shape[0]
    heads = KEY_VALUE_HEADS // 2
    window = assign.shape[0] // 2 + 1
    docs = lengths.shape[0]
    buffers = [
        pltpu.VMEM((chips, 2, 2, span, HEAD_SIZE), jnp.bfloat16) for _ in range(2 * heads)
    ]
    smem = pl.BlockSpec(memory_space=pltpu.SMEM)
    anywhere = pl.BlockSpec(memory_space=pl.ANY)
    dma = pltpu.SemaphoreType.DMA
    return pl.pallas_call(
        functools.partial(kernel, chips, window, docs),
        out_shape=jax.ShapeDtypeStruct(queries.shape, queries.dtype),
        in_specs=[smem, smem, anywhere, anywhere, anywhere],
        out_specs=pl.BlockSpec(memory_space=pltpu.VMEM),
        scratch_shapes=[
            *buffers,
            pltpu.VMEM(queries.shape, queries.dtype),
            pltpu.VMEM((2, window * span, HEAD_SIZE), jnp.bfloat16),
            pltpu.VMEM((2, window * span, HEAD_SIZE), jnp.bfloat16),
            pltpu.VMEM((span, window * span), jnp.float32),
            dma(()),
            dma((heads,)),
            dma((heads, 2, 2 * chips)),
            dma((heads,)),
            dma((heads,)),
            dma((heads,)),
            dma((heads,)),
        ],
        compiler_params=pltpu.CompilerParams(
            collective_id=0, has_side_effects=True, vmem_limit_bytes=60 * 1024 * 1024
        ),
    )(lengths, assign, queries, keys, values)


def solution(mesh):
    rows = P(("group", "seq", "head"), None)
    return jax.shard_map(
        functools.partial(local, mesh.shape["seq"]),
        mesh=mesh,
        in_specs=(rows, rows, rows, P("group"), P("group")),
        out_specs=rows,
        check_vma=False,
    )
```
